32 devices in a mesh: seq: 16 (over z, y, x), slide: 2 (over core).
Axes of the slice: x: 2, y: 2, z: 4, core: 2. Of those that a mesh axis runs over, the one named last changes fastest.
Arguments:
- tile_embed: bfloat16 [16384, 768], P(('slide', 'seq')), parts along dimension 0, may hold values from -6 to 6
- valid_tiles: int32 [2], P('slide'), parts along dimension 0, may hold values from 4096 to 8192
- offsets: int32 [16], replicated, may hold values from 0 to 15
- norm_gain: float32 [768], replicated, may hold values from 0.1 to 1.9
- w_qkv: bfloat16 [768, 2304], replicated
- sub_gain: float32 [768], replicated, may hold values from 0.1 to 1.9
- w_out: bfloat16 [768, 768], replicated, may hold values from -0.21875 to 0.21875
Outputs:
- encoded: bfloat16 [16384, 768], P(('slide', 'seq')), parts along dimension 0
The draws below stay inside these ranges and needn't reach their ends.
There are 2 independent parts, one for each index of `slide`. The reference program is written for one: setup_inputs(seed, part) draws one part's arguments, and reference() takes and returns one part's arrays. A program takes and returns all parts, laid end to end along the dimension named above; an argument that names none is the same for every part. Nothing has to cross between parts.
All inputs are finite; a program needn't handle non-finite values.
Results may differ from the reference program's by a relative error of at most 0.0078.
Values may be sent and summed in bfloat16 or wider, within the bound.
A program may use at most 128 MiB of HBM per device.

```python
import jax
import jax.numpy as jnp
from jax import lax

D = 768
HEADS = 16
DEVICE_TOKENS = 512
SLIDE_TOKENS = 8192
NEAR_SPAN = 2
MIDDLE_DILATION = 4
FAR_DILATION = 16
MIDDLE_SPAN = 4
FAR_SEGMENT_SPAN = 8
N_SEQ = 16


def draw_w_qkv(key, part):
    key_query = jax.random.fold_in(key, 11)
    key_keys = jax.random.fold_in(key, 12)
    key_values = jax.random.fold_in(key, 13)
    spread_scale = D ** (-0.5)
    query_w = jax.random.normal(key_query, (D, D), jnp.float32) * spread_scale
    value_w = jax.random.normal(key_values, (D, D), jnp.float32) * spread_scale
    key_w = jax.random.normal(key_keys, (D, D), jnp.float32) * spread_scale
    return jnp.concatenate([query_w, key_w, value_w], axis=1).astype(jnp.bfloat16)


def with_ends(entries, key, least, high):
    extent = entries.shape
    spot = [jax.random.randint(jax.random.fold_in(key, axis), (), 0, extent[axis]) for axis in range(len(extent))]
    entries = entries.at[tuple(spot)].set(least)
    longest = extent.index(max(extent))
    spot[longest] = (spot[longest] + 1) % extent[longest]
    return entries.at[tuple(spot)].set(high)


def block_levels(own_key, extent, shards, low, top_value):
    def one(position, parts):
        steps = jax.random.uniform(jax.random.fold_in(jax.random.fold_in(own_key, 6), position), (parts,), jnp.float32, low / len(shards), top_value / len(shards))
        return jnp.repeat(jnp.exp(steps), extent[position] // parts).reshape((-1,) + (1,) * (len(extent) - position - 1))

    loudness = one(*shards[0])
    for cut in shards[1:]:
        loudness = loudness * one(*cut)
    return loudness


def noise(stream_key, dims, spread, bound, shards=(), kind=jnp.bfloat16):
    drawn = jax.random.normal(stream_key, dims, jnp.float32) * spread
    if len(shards) > 0:
        drawn = block_levels(stream_key, dims, shards, -0.22, 0.18) * drawn
    return jnp.clip(drawn, min=-bound, max=bound).astype(kind)


def setup_inputs(seed: int = 0, part: int = 0) -> dict:
    key_list = jax.random.split(jax.random.key(seed), 8)
    own_keys = jax.random.split(jax.random.fold_in(key_list[7], part), 8)
    return {
        "tile_embed": noise(own_keys[0], (SLIDE_TOKENS, D), 1.0, 6.0, ((0, 16),)),
        "valid_tiles": jax.random.randint(own_keys[1], (1,), SLIDE_TOKENS // 2, SLIDE_TOKENS + 1).astype(jnp.int32),
        "offsets": with_ends(jax.random.randint(key_list[2], (HEADS,), 0, 16), jax.random.fold_in(key_list[2], 1), 0, 15).astype(jnp.int32),
        "norm_gain": jnp.clip(1.0 + 0.18 * jax.random.normal(key_list[3], (D,), jnp.float32), 0.1, 1.9),
        "w_qkv": draw_w_qkv(jax.random.fold_in(key_list[7], 71), part),
        "sub_gain": jnp.clip(1.0 + 0.18 * jax.random.normal(key_list[5], (D,), jnp.float32), 0.1, 1.9),
        "w_out": noise(key_list[6], (D, D), D ** -0.5, 0.21875),
    }


NEGATIVE = -1e+30
EPSILON = 1e-05

def layer_norm(matrix, gain_row):
    average = lax.optimization_barrier(jnp.mean(matrix, axis=-1, keepdims=True))
    centred = matrix - average
    variance = lax.optimization_barrier(jnp.mean(centred * centred, axis=-1, keepdims=True))
    return centred * lax.rsqrt(variance + EPSILON) * gain_row

def attend(packed):
    query_rows, key_rows, value_rows, key_alive = packed
    scores = jnp.dot(query_rows, key_rows.T, preferred_element_type=jnp.float32) * query_rows.shape[-1] ** (-0.5)
    scores = jnp.where(key_alive[None, :], scores, NEGATIVE)
    row_max = lax.optimization_barrier(jnp.max(scores, axis=1))
    weights = jnp.where(key_alive[None, :], jnp.exp(scores - row_max[:, None]), 0.0)
    row_sum = lax.optimization_barrier(jnp.sum(weights, axis=1))
    numerator = jnp.dot(weights.astype(jnp.bfloat16), value_rows, preferred_element_type=jnp.float32)
    return (row_max, row_sum, numerator)

def branch(query_rows, key_rows, value_rows, offsets, valid_tile_count, seg_len, dilation):
    head_count, length, head_size = query_rows.shape
    segments = length // seg_len
    per_segment = seg_len // dilation
    chosen_mod = (offsets % dilation).astype(jnp.int32)
    picker = jnp.broadcast_to(chosen_mod[:, None, None, None, None], (head_count, segments, per_segment, 1, head_size))

    def select(matrix):
        tiled = matrix.reshape(head_count, segments, per_segment, dilation, head_size)
        return jnp.take_along_axis(tiled, picker, axis=3)[:, :, :, 0, :].reshape(head_count * segments, per_segment, head_size)
    positions = jnp.arange(segments, dtype=jnp.int32)[None, :, None] * seg_len + jnp.arange(per_segment, dtype=jnp.int32)[None, None, :] * dilation + chosen_mod[:, None, None]
    key_alive = (positions < valid_tile_count).reshape(head_count * segments, per_segment)
    row_max, row_sum, numerator = lax.map(attend, (select(query_rows), select(key_rows), select(value_rows), key_alive))
    onehot = jnp.arange(dilation, dtype=jnp.int32)[None, :] == chosen_mod[:, None]
    row_max = jnp.where(onehot[:, None, None, :], row_max.reshape(head_count, segments, per_segment, 1), NEGATIVE)
    row_sum = jnp.where(onehot[:, None, None, :], row_sum.reshape(head_count, segments, per_segment, 1), 0.0)
    numerator = jnp.where(onehot[:, None, None, :, None], numerator.reshape(head_count, segments, per_segment, 1, head_size), 0.0)
    return (row_max.reshape(head_count, length), row_sum.reshape(head_count, length), numerator.reshape(head_count, length, head_size))

def reference(tile_embed, valid_tiles, offsets, norm_gain, w_qkv, sub_gain, w_out):
    relaid = tile_embed.reshape(N_SEQ, DEVICE_TOKENS, D).transpose(1, 0, 2).reshape(SLIDE_TOKENS, D)
    normed = layer_norm(relaid.astype(jnp.float32), norm_gain).astype(jnp.bfloat16)
    projected = jnp.dot(normed, w_qkv, preferred_element_type=jnp.float32).astype(jnp.bfloat16)
    triple = projected.reshape(SLIDE_TOKENS, 3, HEADS, D // HEADS).transpose(1, 2, 0, 3)
    valid_tile_count = valid_tiles[0]
    exchange_plans = [(NEAR_SPAN * DEVICE_TOKENS, 1), (MIDDLE_SPAN * DEVICE_TOKENS, MIDDLE_DILATION), (FAR_SEGMENT_SPAN * DEVICE_TOKENS, FAR_DILATION), (SLIDE_TOKENS, FAR_DILATION)]
    branch_list = [branch(triple[0], triple[1], triple[2], offsets, valid_tile_count, seg_len, dilation) for seg_len, dilation in exchange_plans]
    highest = branch_list[0][0]
    for result in branch_list[1:]:
        highest = jnp.maximum(highest, result[0])
    denom = jnp.zeros_like(highest)
    numer_all = jnp.zeros_like(branch_list[0][2])
    for result in branch_list:
        factor = jnp.exp(result[0] - highest)
        denom = denom + factor * result[1]
        numer_all = numer_all + factor[:, :, None] * result[2]
    attended = (numer_all / jnp.maximum(denom, 1.0)[:, :, None]).astype(jnp.bfloat16)
    flattened = attended.transpose(1, 0, 2).reshape(SLIDE_TOKENS, D)
    sub_normed = layer_norm(flattened.astype(jnp.float32), sub_gain).astype(jnp.bfloat16)
    return (relaid.astype(jnp.float32) + jnp.dot(sub_normed, w_out, preferred_element_type=jnp.float32)).astype(jnp.bfloat16)
```

```python
import functools

import jax
import jax.numpy as jnp
import numpy as np
from jax import lax
from jax.experimental import pallas as pl
from jax.experimental.pallas import tpu as pltpu
from jax.sharding import PartitionSpec as P

MIDDLE_DILATION = 4
FAR_DILATION = 16
NEGATIVE = -1e30
EPSILON = 1e-05
LOG2E = 1.4426950408889634
AUG = 16
VMEM_LIMIT = 60 * 1024 * 1024


def layer_norm_rows(x, gain):
    average = jnp.mean(x, axis=-1, keepdims=True)
    centred = x - average
    variance = jnp.mean(centred * centred, axis=-1, keepdims=True)
    return centred * lax.rsqrt(variance + EPSILON) * gain


def project_into(dst, x_ref, gain_ref, w_ref, chunk, skip=0):
    normed = layer_norm_rows(x_ref[...].astype(jnp.float32), gain_ref[...]).astype(jnp.bfloat16)

    @pl.loop(0, (w_ref.shape[0] - skip) // chunk)
    def _(i):
        rows = pl.ds(pl.multiple_of(i * chunk, chunk), chunk)
        dst[rows, :] = lax.dot_general(
            w_ref[pl.ds(pl.multiple_of(i * chunk + skip, chunk), chunk), :], normed, (((1,), (1,)), ((), ())), preferred_element_type=jnp.float32
        ).astype(jnp.bfloat16)


def project_kernel(heads, offs, x_ref, gain_ref, w_ref, proj_ref, mid_ref, far_ref, far_scr):
    rows, width = x_ref.shape
    size = width // heads
    lanes = rows // MIDDLE_DILATION
    few = rows // FAR_DILATION
    project_into(proj_ref, x_ref, gain_ref, w_ref, 256)
    src = lax.broadcasted_iota(jnp.int32, (lanes, lanes), 0)
    dst = lax.broadcasted_iota(jnp.int32, (lanes, lanes), 1)
    for head in range(heads):
        phase = offs[head] % FAR_DILATION
        quarter = phase % MIDDLE_DILATION
        shift = (phase // MIDDLE_DILATION) * few
        pick = ((src == dst + shift) & (dst < few)).astype(jnp.bfloat16)
        for part in range(2):
            base = part * width + head * size
            block = proj_ref[
                width + base : width + base + size,
                pl.ds(pl.multiple_of(quarter * lanes, lanes), lanes),
            ]
            mid_ref[base : base + size, :] = block
            far_scr[base : base + size, :] = jnp.dot(
                block, pick, preferred_element_type=jnp.float32
            )
    far_ref[...] = far_scr[...].T[:few].astype(jnp.bfloat16)


def aug_rows(first, lanes, second=None):
    spot = lax.broadcasted_iota(jnp.int32, (AUG, lanes), 0)
    rows = jnp.where(spot == 0, first, 0.0)
    if second is not None:
        rows = jnp.where(spot == 1, second, rows)
    return rows.astype(jnp.bfloat16)


def weighted_values(value, weight):
    scaled = (value.astype(jnp.float32) * weight).astype(jnp.bfloat16)
    return jnp.concatenate([scaled, aug_rows(weight, value.shape[1])], axis=0)


def scores_of(keys, queries):
    return lax.dot_general(
        keys, queries, (((0,), (0,)), ((), ())), preferred_element_type=jnp.float32
    )


def own_kernel(scale, per_step, size, valid, q_ref, k_ref, v_ref, pos_ref, out_ref):
    lanes = q_ref.shape[1]
    alive = pos_ref[...] + lax.axis_index("seq") * lanes < valid[0]
    bias = aug_rows(jnp.where(alive, 0.0, NEGATIVE), lanes)
    weight = jnp.where(alive, 1.0, 0.0)
    unit = aug_rows(jnp.ones((1, lanes), jnp.float32), lanes)
    for i in range(per_step):
        part = slice(i * size, (i + 1) * size)
        scores = scores_of(
            jnp.concatenate([k_ref[part, :], bias], axis=0),
            jnp.concatenate([q_ref[part, :], unit], axis=0),
        )
        top = jnp.max(scores, axis=0, keepdims=True)
        p = jnp.exp2((scores - top) * scale).astype(jnp.bfloat16)
        base = i * (size + AUG)
        out_ref[base : base + size + AUG, :] = jnp.dot(
            weighted_values(v_ref[part, :], weight), p, preferred_element_type=jnp.float32
        )
        out_ref[base + size + 1 : base + size + 2, :] = top


def rest_kernel(
    heads, scale, per_step, far_span, middle, offs, valid,
    x_ref, xp_ref, gain_ref, w_ref, q_ref, k_ref, v_ref, own_ref, ppos_ref,
    *rest,
):
    others = middle - 2
    midk, midv = rest[:others], rest[others : 2 * others]
    far_ref, extra_ref, subgain_ref, wout_ref, out_ref, kvp, far_t, o_scr, att = rest[2 * others :]
    rows, width = x_ref.shape
    size = width // heads
    lanes = rows // MIDDLE_DILATION
    few = rows // FAR_DILATION
    step = pl.program_id(0)

    @pl.when(step == 0)
    def _():
        project_into(kvp, xp_ref, gain_ref, w_ref, 256, width)
        for i in range(far_ref.shape[0] // 128):
            far_t[:, i * 128 : (i + 1) * 128] = far_ref[i * 128 : (i + 1) * 128, :].T

    me = lax.axis_index("seq")
    alive = ppos_ref[...] + (me ^ 1) * rows < valid[0]
    bias = aug_rows(jnp.where(alive, 0.0, NEGATIVE), rows)
    weight = jnp.where(alive, 1.0, 0.0)
    unit = aug_rows(jnp.ones((1, rows), jnp.float32), rows)
    is_far = extra_ref[1:2, :]
    device = jnp.where(is_far == 1, extra_ref[2:3, :], extra_ref[2:3, :] ^ me)
    start = extra_ref[0:1, :] + device * rows
    times = jnp.where((is_far == 1) & (extra_ref[3:4, :] == me // far_span), 2, 1)
    lane = lax.broadcasted_iota(jnp.int32, (1, lanes), 1)
    for i in range(per_step):
        head = step * per_step + i
        part = slice(i * size, (i + 1) * size)
        base = i * (size + AUG)
        both = slice(base, base + size + AUG)
        phase = offs[head] % FAR_DILATION
        quarter = phase % MIDDLE_DILATION
        cols = pl.ds(pl.multiple_of(quarter * lanes, lanes), lanes)
        krows = pl.ds(pl.multiple_of(head * size, AUG), size)
        vrows = pl.ds(pl.multiple_of(width + head * size, AUG), size)

        scores = scores_of(
            jnp.concatenate([kvp[krows, :], bias], axis=0),
            jnp.concatenate([q_ref[part, :], unit], axis=0),
        )
        own = own_ref[both, :]
        own_top = own[size + 1 : size + 2, :]
        top = jnp.maximum(own_top, jnp.max(scores, axis=0, keepdims=True))
        p = jnp.exp2((scores - top) * scale).astype(jnp.bfloat16)
        o_scr[both, :] = own * jnp.exp2((own_top - top) * scale) + jnp.dot(
            weighted_values(kvp[vrows, :], weight), p, preferred_element_type=jnp.float32
        )
        o_scr[base + size + 1 : base + size + 2, :] = top

        keys = jnp.concatenate(
            [k_ref[part, cols], kvp[krows, cols]]
            + [midk[g][part, :] for g in range(others)]
            + [far_t[krows, :]],
            axis=1,
        )
        values = jnp.concatenate(
            [v_ref[part, cols], kvp[vrows, cols]]
            + [midv[g][part, :] for g in range(others)]
            + [far_t[vrows, :]],
            axis=1,
        )
        spot = start + jnp.where(is_far == 1, phase, quarter)
        live = spot < valid[0]
        count = jnp.where(live, times, 0).astype(jnp.float32)
        keys = jnp.concatenate(
            [
                keys,
                aug_rows(
                    jnp.where(live, 0.0, NEGATIVE), keys.shape[1], is_far.astype(jnp.float32)
                ),
            ],
            axis=0,
        )
        mine = lane // few == phase // MIDDLE_DILATION
        queries = jnp.concatenate(
            [
                q_ref[part, cols],
                aug_rows(
                    jnp.ones((1, lanes), jnp.float32), lanes, jnp.where(mine, 0.0, NEGATIVE)
                ),
            ],
            axis=0,
        )
        more = scores_of(keys, queries)
        had = o_scr[both, cols]
        had_top = had[size + 1 : size + 2, :]
        new_top = jnp.maximum(had_top, jnp.max(more, axis=0, keepdims=True))
        p = jnp.exp2((more - new_top) * scale).astype(jnp.bfloat16)
        total = had * jnp.exp2((had_top - new_top) * scale) + jnp.dot(
            weighted_values(values, count), p, preferred_element_type=jnp.float32
        )
        o_scr[both, cols] = jnp.where(new_top > 0.5 * NEGATIVE, total, 0.0)
        done = o_scr[both, :]
        result = done[:size] / jnp.maximum(done[size : size + 1], 1.0)
        att[pl.ds(pl.multiple_of(head * size, AUG), size), :] = result.astype(jnp.bfloat16)

    @pl.when(step == pl.num_programs(0) - 1)
    def _():
        attended = att[...].astype(jnp.float32)
        average = jnp.mean(attended, axis=0, keepdims=True)
        centred = attended - average
        variance = jnp.mean(centred * centred, axis=0, keepdims=True)
        normed = centred * lax.rsqrt(variance + EPSILON) * subgain_ref[...]
        projected = jnp.dot(
            normed.T.astype(jnp.bfloat16), wout_ref[...], preferred_element_type=jnp.float32
        )
        out_ref[...] = (x_ref[...].astype(jnp.float32) + projected).astype(jnp.bfloat16)


def body(tile_embed, valid_tiles, offsets, norm_gain, w_qkv, sub_gain, w_out):
    devices = lax.axis_size("seq")
    me = lax.axis_index("seq")
    rows, width = tile_embed.shape
    heads = offsets.shape[0]
    size = width // heads
    lanes = rows // MIDDLE_DILATION
    few = rows // FAR_DILATION
    each = rows // devices
    middle = max(4, devices // 16)
    far_span = max(8, devices // 4)
    per_step = 2
    steps = heads // per_step
    scale = float(size) ** -0.5 * LOG2E

    w_t = w_qkv.T
    pieces = tile_embed.reshape(devices, each, width)
    arrived = lax.all_to_all(pieces, "seq", split_axis=0, concat_axis=0, tiled=True)
    groups = devices // FAR_DILATION
    x = arrived.reshape(groups, 4, 4, each, width).transpose(2, 1, 0, 3, 4).reshape(rows, width)
    xp = lax.ppermute(x, "seq", [(d, d ^ 1) for d in range(devices)])

    whole = lambda *shape: pl.BlockSpec(shape, lambda *_: (0,) * len(shape))
    smem = pl.BlockSpec(memory_space=pltpu.SMEM)
    gain = norm_gain.reshape(1, width)

    proj, mid, far = pl.pallas_call(
        functools.partial(project_kernel, heads),
        out_shape=(
            jax.ShapeDtypeStruct((3 * width, rows), jnp.bfloat16),
            jax.ShapeDtypeStruct((2 * width, lanes), jnp.bfloat16),
            jax.ShapeDtypeStruct((few, 2 * width), jnp.bfloat16),
        ),
        in_specs=[smem] + [pl.BlockSpec(memory_space=pltpu.VMEM)] * 3,
        out_specs=(pl.BlockSpec(memory_space=pltpu.VMEM),) * 3,
        scratch_shapes=[pltpu.VMEM((2 * width, lanes), jnp.float32)],
        compiler_params=pltpu.CompilerParams(vmem_limit_bytes=VMEM_LIMIT),
        cost_estimate=pl.CostEstimate(
            flops=6 * rows * width * width, bytes_accessed=12 * width * width, transcendentals=0
        ),
        name="project",
    )(offsets, x, gain, w_t)

    mids = [
        lax.ppermute(mid, "seq", [(d, d ^ g) for d in range(devices)]) for g in range(2, middle)
    ]
    far_all = lax.all_gather(far, "seq", axis=0, tiled=True)

    local = np.arange(rows, dtype=np.int32).reshape(each, groups, 4, 4).transpose(3, 2, 1, 0)
    local = local.reshape(1, rows)
    seats = np.arange(devices, dtype=np.int32)
    mid_rows = [np.tile(local[0, :lanes], middle), np.zeros(middle * lanes, np.int32),
                np.repeat(np.arange(middle, dtype=np.int32), lanes),
                np.zeros(middle * lanes, np.int32)]
    far_rows = [np.tile(local[0, :few], devices), np.ones(devices * few, np.int32),
                np.repeat(seats, few), np.repeat(seats // far_span, few)]
    extra = np.concatenate([np.stack(mid_rows), np.stack(far_rows)], axis=1)
    extra_count = extra.shape[1]

    strip = per_step * size
    out_strip = per_step * (size + AUG)
    block = lambda part: pl.BlockSpec((strip, rows), lambda h: (part * steps + h, 0))
    own = pl.pallas_call(
        functools.partial(own_kernel, scale, per_step, size),
        grid=(steps,),
        out_shape=jax.ShapeDtypeStruct((heads * (size + AUG), rows), jnp.float32),
        in_specs=[smem, block(0), block(1), block(2), whole(1, rows)],
        out_specs=pl.BlockSpec((out_strip, rows), lambda h: (h, 0)),
        compiler_params=pltpu.CompilerParams(vmem_limit_bytes=VMEM_LIMIT),
        cost_estimate=pl.CostEstimate(
            flops=16 * rows * rows * width, bytes_accessed=8 * rows * width,
            transcendentals=heads * rows * rows,
        ),
        name="own_keys",
    )(valid_tiles, proj, proj, proj, jnp.asarray(local))

    out = pl.pallas_call(
        functools.partial(rest_kernel, heads, scale, per_step, far_span, middle),
        grid=(steps,),
        out_shape=jax.ShapeDtypeStruct((rows, width), jnp.bfloat16),
        in_specs=[
            smem, smem,
            whole(rows, width), whole(rows, width), whole(1, width), whole(3 * width, width),
            block(0), block(1), block(2),
            pl.BlockSpec((out_strip, rows), lambda h: (h, 0)),
            whole(1, rows),
            *[pl.BlockSpec((strip, lanes), lambda h: (h, 0))] * len(mids),
            *[pl.BlockSpec((strip, lanes), lambda h: (steps + h, 0))] * len(mids),
            whole(devices * few, 2 * width), whole(4, extra_count),
            whole(width, 1), whole(width, width),
        ],
        out_specs=whole(rows, width),
        scratch_shapes=[
            pltpu.VMEM((2 * width, rows), jnp.bfloat16),
            pltpu.VMEM((2 * width, devices * few), jnp.bfloat16),
            pltpu.VMEM((out_strip, rows), jnp.float32),
            pltpu.VMEM((width, rows), jnp.bfloat16),
        ],
        compiler_params=pltpu.CompilerParams(vmem_limit_bytes=VMEM_LIMIT),
        cost_estimate=pl.CostEstimate(
            flops=24 * rows * rows * width, bytes_accessed=20 * rows * width,
            transcendentals=heads * rows * rows,
        ),
        name="rest",
    )(
        offsets, valid_tiles, x, xp, gain, w_t, proj, proj, proj, own, jnp.asarray(local),
        *mids, *mids, far_all, jnp.asarray(extra), sub_gain.reshape(width, 1), w_out,
    )
    return (
        out.reshape(4, 4, groups, each, width).transpose(3, 2, 1, 0, 4).reshape(rows, width)
    )


def solution(mesh):
    return jax.shard_map(
        body,
        mesh=mesh,
        in_specs=(P(("slide", "seq"), None), P("slide"), P(), P(), P(), P(), P()),
        out_specs=P(("slide", "seq"), None),
        check_vma=False,
    )
```

```python
import functools

import jax
import jax.numpy as jnp
import numpy as np
from jax import lax
from jax.experimental import pallas as pl
from jax.experimental.pallas import tpu as pltpu
from jax.sharding import PartitionSpec as P

MIDDLE_DILATION = 4
FAR_DILATION = 16
NEGATIVE = -1e30
EPSILON = 1e-05
LOG2E = 1.4426950408889634
AUG = 16
VMEM_LIMIT = 60 * 1024 * 1024


def layer_norm_rows(x, gain):
    average = jnp.mean(x, axis=-1, keepdims=True)
    centred = x - average
    variance = jnp.mean(centred * centred, axis=-1, keepdims=True)
    return centred * lax.rsqrt(variance + EPSILON) * gain


def project_into(dst, x_ref, gain_ref, w_ref, chunk, skip=0):
    normed = layer_norm_rows(x_ref[...].astype(jnp.float32), gain_ref[...]).astype(jnp.bfloat16)

    @pl.loop(0, (w_ref.shape[0] - skip) // chunk)
    def _(i):
        rows = pl.ds(pl.multiple_of(i * chunk, chunk), chunk)
        dst[rows, :] = lax.dot_general(
            w_ref[pl.ds(pl.multiple_of(i * chunk + skip, chunk), chunk), :], normed, (((1,), (1,)), ((), ())), preferred_element_type=jnp.float32
        ).astype(jnp.bfloat16)


def project_kernel(heads, offs, x_ref, gain_ref, w_ref, proj_ref, mid_ref, fark_ref, farv_ref, far_scr):
    rows, width = x_ref.shape
    size = width // heads
    lanes = rows // MIDDLE_DILATION
    few = rows // FAR_DILATION
    project_into(proj_ref, x_ref, gain_ref, w_ref, 256)
    src = lax.broadcasted_iota(jnp.int32, (lanes, lanes), 0)
    dst = lax.broadcasted_iota(jnp.int32, (lanes, lanes), 1)
    for head in range(heads):
        phase = offs[head] % FAR_DILATION
        quarter = phase % MIDDLE_DILATION
        shift = (phase // MIDDLE_DILATION) * few
        pick = ((src == dst + shift) & (dst < few)).astype(jnp.bfloat16)
        for part in range(2):
            base = part * width + head * size
            block = proj_ref[
                width + base : width + base + size,
                pl.ds(pl.multiple_of(quarter * lanes, lanes), lanes),
            ]
            mid_ref[base : base + size, :] = block
            far_scr[base : base + size, :] = jnp.dot(
                block, pick, preferred_element_type=jnp.float32
            )
    fark_ref[...] = far_scr[:width, :].T[:few].astype(jnp.bfloat16)
    farv_ref[...] = far_scr[width:, :].T[:few].astype(jnp.bfloat16)


def aug_rows(first, lanes, second=None):
    spot = lax.broadcasted_iota(jnp.int32, (AUG, lanes), 0)
    rows = jnp.where(spot == 0, first, 0.0)
    if second is not None:
        rows = jnp.where(spot == 1, second, rows)
    return rows.astype(jnp.bfloat16)


def weighted_values(value, weight):
    scaled = (value.astype(jnp.float32) * weight).astype(jnp.bfloat16)
    return jnp.concatenate([scaled, aug_rows(weight, value.shape[1])], axis=0)


def scores_of(keys, queries):
    return lax.dot_general(
        keys, queries, (((0,), (0,)), ((), ())), preferred_element_type=jnp.float32
    )


def own_kernel(scale, per_step, size, valid, q_ref, k_ref, v_ref, pos_ref, out_ref):
    lanes = q_ref.shape[1]
    alive = pos_ref[...] + lax.axis_index("seq") * lanes < valid[0]
    bias = aug_rows(jnp.where(alive, 0.0, NEGATIVE), lanes)
    weight = jnp.where(alive, 1.0, 0.0)
    unit = aug_rows(jnp.ones((1, lanes), jnp.float32), lanes)
    for i in range(per_step):
        part = slice(i * size, (i + 1) * size)
        scores = scores_of(
            jnp.concatenate([k_ref[part, :], bias], axis=0),
            jnp.concatenate([q_ref[part, :], unit], axis=0),
        )
        top = jnp.max(scores, axis=0, keepdims=True)
        p = jnp.exp2((scores - top) * scale).astype(jnp.bfloat16)
        base = i * (size + AUG)
        out_ref[base : base + size + AUG, :] = jnp.dot(
            weighted_values(v_ref[part, :], weight), p, preferred_element_type=jnp.float32
        )
        out_ref[base + size + 1 : base + size + 2, :] = top


def rest_kernel(
    heads, scale, per_step, far_span, middle, offs, valid,
    x_ref, xp_ref, gain_ref, w_ref, q_ref, k_ref, v_ref, own_ref, ppos_ref,
    *rest,
):
    others = middle - 2
    midk, midv = rest[:others], rest[others : 2 * others]
    fark_ref, farv_ref, extra_ref, subgain_ref, wout_ref = rest[2 * others : 2 * others + 5]
    out_ref, kvp, far_t, o_scr, att = rest[2 * others + 5 :]
    rows, width = x_ref.shape
    size = width // heads
    lanes = rows // MIDDLE_DILATION
    few = rows // FAR_DILATION
    step = pl.program_id(0)

    @pl.when(step == 0)
    def _():
        project_into(kvp, xp_ref, gain_ref, w_ref, 256, width)
        for i in range(fark_ref.shape[0] // 128):
            far_t[:width, i * 128 : (i + 1) * 128] = fark_ref[i * 128 : (i + 1) * 128, :].T
            far_t[width:, i * 128 : (i + 1) * 128] = farv_ref[i * 128 : (i + 1) * 128, :].T

    me = lax.axis_index("seq")
    alive = ppos_ref[...] + (me ^ 1) * rows < valid[0]
    bias = aug_rows(jnp.where(alive, 0.0, NEGATIVE), rows)
    weight = jnp.where(alive, 1.0, 0.0)
    unit = aug_rows(jnp.ones((1, rows), jnp.float32), rows)
    is_far = extra_ref[1:2, :]
    device = extra_ref[2:3, :] ^ me
    start = extra_ref[0:1, :] + device * rows
    times = jnp.where((is_far == 1) & (device // far_span == me // far_span), 2, 1)
    lane = lax.broadcasted_iota(jnp.int32, (1, lanes), 1)
    for i in range(per_step):
        head = step * per_step + i
        part = slice(i * size, (i + 1) * size)
        base = i * (size + AUG)
        both = slice(base, base + size + AUG)
        phase = offs[head] % FAR_DILATION
        quarter = phase % MIDDLE_DILATION
        cols = pl.ds(pl.multiple_of(quarter * lanes, lanes), lanes)
        krows = pl.ds(pl.multiple_of(head * size, AUG), size)
        vrows = pl.ds(pl.multiple_of(width + head * size, AUG), size)

        scores = scores_of(
            jnp.concatenate([kvp[krows, :], bias], axis=0),
            jnp.concatenate([q_ref[part, :], unit], axis=0),
        )
        own = own_ref[both, :]
        own_top = own[size + 1 : size + 2, :]
        top = jnp.maximum(own_top, jnp.max(scores, axis=0, keepdims=True))
        p = jnp.exp2((scores - top) * scale).astype(jnp.bfloat16)
        o_scr[both, :] = own * jnp.exp2((own_top - top) * scale) + jnp.dot(
            weighted_values(kvp[vrows, :], weight), p, preferred_element_type=jnp.float32
        )
        o_scr[base + size + 1 : base + size + 2, :] = top

        keys = jnp.concatenate(
            [k_ref[part, cols], kvp[krows, cols]]
            + [midk[g][part, :] for g in range(others)]
            + [far_t[krows, :]],
            axis=1,
        )
        values = jnp.concatenate(
            [v_ref[part, cols], kvp[vrows, cols]]
            + [midv[g][part, :] for g in range(others)]
            + [far_t[vrows, :]],
            axis=1,
        )
        spot = start + jnp.where(is_far == 1, phase, quarter)
        live = spot < valid[0]
        count = jnp.where(live, times, 0).astype(jnp.float32)
        keys = jnp.concatenate(
            [
                keys,
                aug_rows(
                    jnp.where(live, 0.0, NEGATIVE), keys.shape[1], is_far.astype(jnp.float32)
                ),
            ],
            axis=0,
        )
        mine = lane // few == phase // MIDDLE_DILATION
        queries = jnp.concatenate(
            [
                q_ref[part, cols],
                aug_rows(
                    jnp.ones((1, lanes), jnp.float32), lanes, jnp.where(mine, 0.0, NEGATIVE)
                ),
            ],
            axis=0,
        )
        more = scores_of(keys, queries)
        had = o_scr[both, cols]
        had_top = had[size + 1 : size + 2, :]
        new_top = jnp.maximum(had_top, jnp.max(more, axis=0, keepdims=True))
        p = jnp.exp2((more - new_top) * scale).astype(jnp.bfloat16)
        total = had * jnp.exp2((had_top - new_top) * scale) + jnp.dot(
            weighted_values(values, count), p, preferred_element_type=jnp.float32
        )
        o_scr[both, cols] = jnp.where(new_top > 0.5 * NEGATIVE, total, 0.0)
        done = o_scr[both, :]
        result = done[:size] / jnp.maximum(done[size : size + 1], 1.0)
        att[pl.ds(pl.multiple_of(head * size, AUG), size), :] = result.astype(jnp.bfloat16)

    @pl.when(step == pl.num_programs(0) - 1)
    def _():
        attended = att[...].astype(jnp.float32)
        average = jnp.mean(attended, axis=0, keepdims=True)
        centred = attended - average
        variance = jnp.mean(centred * centred, axis=0, keepdims=True)
        normed = centred * lax.rsqrt(variance + EPSILON) * subgain_ref[...]
        projected = jnp.dot(
            normed.T.astype(jnp.bfloat16), wout_ref[...], preferred_element_type=jnp.float32
        )
        out_ref[...] = (x_ref[...].astype(jnp.float32) + projected).astype(jnp.bfloat16)


def doubled(rows, bit, devices):
    pairs = [(d, d ^ (1 << bit)) for d in range(devices)]
    return jnp.concatenate([rows, lax.ppermute(rows, "seq", pairs)], axis=0)


def body(tile_embed, valid_tiles, offsets, norm_gain, w_qkv, sub_gain, w_out):
    devices = lax.axis_size("seq")
    me = lax.axis_index("seq")
    rows, width = tile_embed.shape
    heads = offsets.shape[0]
    size = width // heads
    lanes = rows // MIDDLE_DILATION
    few = rows // FAR_DILATION
    each = rows // devices
    middle = max(4, devices // 16)
    far_span = max(8, devices // 4)
    per_step = 2
    steps = heads // per_step
    scale = float(size) ** -0.5 * LOG2E

    w_t = w_qkv.T
    pieces = tile_embed.reshape(devices, each, width)
    arrived = lax.all_to_all(pieces, "seq", split_axis=0, concat_axis=0, tiled=True)
    groups = devices // FAR_DILATION
    x = arrived.reshape(groups, 4, 4, each, width).transpose(2, 1, 0, 3, 4).reshape(rows, width)
    xp = lax.ppermute(x, "seq", [(d, d ^ 1) for d in range(devices)])

    whole = lambda *shape: pl.BlockSpec(shape, lambda *_: (0,) * len(shape))
    smem = pl.BlockSpec(memory_space=pltpu.SMEM)
    gain = norm_gain.reshape(1, width)

    proj, mid, far_key, far_value = pl.pallas_call(
        functools.partial(project_kernel, heads),
        out_shape=(
            jax.ShapeDtypeStruct((3 * width, rows), jnp.bfloat16),
            jax.ShapeDtypeStruct((2 * width, lanes), jnp.bfloat16),
            jax.ShapeDtypeStruct((few, width), jnp.bfloat16),
            jax.ShapeDtypeStruct((few, width), jnp.bfloat16),
        ),
        in_specs=[smem] + [pl.BlockSpec(memory_space=pltpu.VMEM)] * 3,
        out_specs=(pl.BlockSpec(memory_space=pltpu.VMEM),) * 4,
        scratch_shapes=[pltpu.VMEM((2 * width, lanes), jnp.float32)],
        compiler_params=pltpu.CompilerParams(vmem_limit_bytes=VMEM_LIMIT),
        cost_estimate=pl.CostEstimate(
            flops=6 * rows * width * width, bytes_accessed=12 * width * width, transcendentals=0
        ),
        name="project",
    )(offsets, x, gain, w_t)

    mids = [
        lax.ppermute(mid, "seq", [(d, d ^ g) for d in range(devices)]) for g in range(2, middle)
    ]
    bits = devices.bit_length() - 1
    for bit in range(bits):
        far_key = doubled(far_key, bit, devices)
        far_value = doubled(far_value, bits - 1 - bit, devices)
    far_value = (
        far_value.reshape((2,) * bits + (few, width))
        .transpose(tuple(reversed(range(bits))) + (bits, bits + 1))
        .reshape(devices * few, width)
    )

    local = np.arange(rows, dtype=np.int32).reshape(each, groups, 4, 4).transpose(3, 2, 1, 0)
    local = local.reshape(1, rows)
    seats = np.arange(devices, dtype=np.int32)
    mid_rows = [np.tile(local[0, :lanes], middle), np.zeros(middle * lanes, np.int32),
                np.repeat(np.arange(middle, dtype=np.int32), lanes)]
    far_rows = [np.tile(local[0, :few], devices), np.ones(devices * few, np.int32),
                np.repeat(seats, few)]
    extra = np.concatenate([np.stack(mid_rows), np.stack(far_rows)], axis=1)
    extra_count = extra.shape[1]

    strip = per_step * size
    out_strip = per_step * (size + AUG)
    block = lambda part: pl.BlockSpec((strip, rows), lambda h: (part * steps + h, 0))
    own = pl.pallas_call(
        functools.partial(own_kernel, scale, per_step, size),
        grid=(steps,),
        out_shape=jax.ShapeDtypeStruct((heads * (size + AUG), rows), jnp.float32),
        in_specs=[smem, block(0), block(1), block(2), whole(1, rows)],
        out_specs=pl.BlockSpec((out_strip, rows), lambda h: (h, 0)),
        compiler_params=pltpu.CompilerParams(vmem_limit_bytes=VMEM_LIMIT),
        cost_estimate=pl.CostEstimate(
            flops=16 * rows * rows * width, bytes_accessed=8 * rows * width,
            transcendentals=heads * rows * rows,
        ),
        name="own_keys",
    )(valid_tiles, proj, proj, proj, jnp.asarray(local))

    out = pl.pallas_call(
        functools.partial(rest_kernel, heads, scale, per_step, far_span, middle),
        grid=(steps,),
        out_shape=jax.ShapeDtypeStruct((rows, width), jnp.bfloat16),
        in_specs=[
            smem, smem,
            whole(rows, width), whole(rows, width), whole(1, width), whole(3 * width, width),
            block(0), block(1), block(2),
            pl.BlockSpec((out_strip, rows), lambda h: (h, 0)),
            whole(1, rows),
            *[pl.BlockSpec((strip, lanes), lambda h: (h, 0))] * len(mids),
            *[pl.BlockSpec((strip, lanes), lambda h: (steps + h, 0))] * len(mids),
            whole(devices * few, width), whole(devices * few, width), whole(3, extra_count),
            whole(width, 1), whole(width, width),
        ],
        out_specs=whole(rows, width),
        scratch_shapes=[
            pltpu.VMEM((2 * width, rows), jnp.bfloat16),
            pltpu.VMEM((2 * width, devices * few), jnp.bfloat16),
            pltpu.VMEM((out_strip, rows), jnp.float32),
            pltpu.VMEM((width, rows), jnp.bfloat16),
        ],
        compiler_params=pltpu.CompilerParams(vmem_limit_bytes=VMEM_LIMIT),
        cost_estimate=pl.CostEstimate(
            flops=24 * rows * rows * width, bytes_accessed=20 * rows * width,
            transcendentals=heads * rows * rows,
        ),
        name="rest",
    )(
        offsets, valid_tiles, x, xp, gain, w_t, proj, proj, proj, own, jnp.asarray(local),
        *mids, *mids, far_key, far_value, jnp.asarray(extra), sub_gain.reshape(width, 1), w_out,
    )
    return (
        out.reshape(4, 4, groups, each, width).transpose(3, 2, 1, 0, 4).reshape(rows, width)
    )


def solution(mesh):
    return jax.shard_map(
        body,
        mesh=mesh,
        in_specs=(P(("slide", "seq"), None), P("slide"), P(), P(), P(), P(), P()),
        out_specs=P(("slide", "seq"), None),
        check_vma=False,
    )
```
